32 devices in a mesh: lat: 16 (over z, y, core), lon: 2 (over x).
Axes of the slice: x: 2, y: 2, z: 4, core: 2. Of those that a mesh axis runs over, the one named last changes fastest.
Arguments:
- features: bfloat16 [256, 128, 512], P('lat', 'lon'), may hold values from -6 to 6
- upstream: bfloat16 [256, 128, 512], P('lat', 'lon'), may hold values from -6 to 6
- kernel: bfloat16 [4608, 512], replicated, may hold values from -0.09375 to 0.09375
Outputs:
- input_grad: bfloat16 [256, 128, 512], P('lat', 'lon')
- direction: float32 [4608, 512], P('lat')
- perturbed: float32 [4608, 512], P('lat')
The draws below stay inside these ranges and needn't reach their ends.
All inputs are finite; a program needn't handle non-finite values.
Results may differ from the reference program's by a relative error of at most 0.0032.
Values may be sent and summed in bfloat16 or wider, within the bound.
A program may use at most 128 MiB of HBM per device.

```python
import jax
import jax.numpy as jnp
from jax import lax

C = 512
NLAT = 256
NLON = 128


def block_levels(stream_key, extent, pieces, low, top_value):
    level, own = 1.0, jax.random.fold_in(stream_key, 6)
    for dim, blocks in pieces:
        draws = jnp.exp(jax.random.uniform(jax.random.fold_in(own, dim), (blocks,), jnp.float32, low / len(pieces), top_value / len(pieces)))
        level = level * jnp.repeat(draws, extent[dim] // blocks).reshape([-1 if axis == dim else 1 for axis in range(len(extent))])
    return level


def centred(key, dims, spread, most, split=(), held_as=jnp.bfloat16):
    entries = spread * jax.random.normal(key, dims, jnp.float32)
    if split:
        entries = entries * block_levels(key, dims, split, -0.22, 0.18)
    return jnp.clip(entries, -most, most).astype(held_as)


def setup_inputs(seed: int = 0) -> dict:
    arg_keys = jax.random.split(jax.random.key(seed), 4)
    return {
        "features": centred(arg_keys[0], (NLAT, NLON, C), 1.0, 6.0, ((0, 16), (1, 2))),
        "upstream": centred(arg_keys[1], (NLAT, NLON, C), 1.0, 6.0, ((0, 16), (1, 2))),
        "kernel": centred(arg_keys[2], (9 * C, C), (9 * C) ** -0.5, 0.09375),
    }


def extend(field):
    wrapped = jnp.concatenate([field[:, -1:], field, field[:, :1]], axis=1)
    return jnp.pad(wrapped, ((1, 1), (0, 0), (0, 0)))

def reference(features, upstream, kernel):
    height, breadth, channels = features.shape
    padded_x = extend(features)
    z = jnp.zeros((height, breadth, channels), jnp.float32)
    for a in range(3):
        for b in range(3):
            t = 3 * a + b
            z = z + jnp.dot(padded_x[a:a + height, b:b + breadth], kernel[t * channels:(t + 1) * channels], preferred_element_type=jnp.float32)
    sig = jax.nn.sigmoid(z)
    slope = (upstream.astype(jnp.float32) * sig * (1.0 + z * (1.0 - sig))).astype(jnp.bfloat16)
    padded_slope = extend(slope)
    back = upstream.astype(jnp.float32)
    blocks = []
    for a in range(3):
        for b in range(3):
            t = 3 * a + b
            piece = padded_slope[2 - a:2 - a + height, 2 - b:2 - b + breadth]
            back = back + lax.dot_general(piece, kernel[t * channels:(t + 1) * channels], (((2,), (1,)), ((), ())), preferred_element_type=jnp.float32)
            blocks.append(lax.dot_general(padded_x[a:a + height, b:b + breadth], slope, (((0, 1), (0, 1)), ((), ())), preferred_element_type=jnp.float32))
    input_grad = back.astype(jnp.bfloat16)
    grad = jnp.concatenate(blocks, axis=0)
    count = 9.0 * channels * channels
    total = jnp.sum(grad * grad)
    direction = grad / jnp.sqrt(total / count + 1e-06)
    perturbed = kernel.astype(jnp.float32) + 0.05 / jnp.sqrt(count) * direction
    return (input_grad, direction, perturbed)
```

```python
import functools

import jax
import jax.numpy as jnp
from jax import lax
from jax.experimental import pallas as pl
from jax.experimental.pallas import tpu as pltpu
from jax.sharding import PartitionSpec as P

MESH = pl.DeviceIdType.MESH


def padded_2(block, sides, width, periodic):
    for axis, dim in sides:
        count = lax.axis_size(axis)
        forward = [(i, i + 1) for i in range(count - 1)]
        if periodic:
            forward.append((count - 1, 0))
        backward = [(target, source) for source, target in forward]
        low = lax.ppermute(
            lax.slice_in_dim(block, block.shape[dim] - width, None, axis=dim), axis, forward
        )
        high = lax.ppermute(lax.slice_in_dim(block, 0, width, axis=dim), axis, backward)
        block = jnp.concatenate([low, block, high], axis=dim)
    return block


def gated(upstream, z):
    sig = jax.nn.sigmoid(z)
    return upstream.astype(jnp.float32) * sig * (1.0 + z * (1.0 - sig))


def slots_in_order(bits):
    order = [0]
    for _ in range(bits):
        order = [2 * v for v in order] + [2 * v + 1 for v in order]
    reverse = lambda v: int(format(v, "b").zfill(bits)[::-1], 2) if bits else 0
    return sorted(order, key=reverse, reverse=True)


def reduce_kernel(n_lat, n_lon, count, *refs):
    grad, own, direction, perturbed, acc, send, recv, beside, squares = refs[:9]
    send_sem, recv_sem, lon_send, lon_recv, sq_send, sq_recv = refs[9:]
    rows, channels = own.shape
    lat = lax.axis_index("lat")
    lon = lax.axis_index("lon")
    stages = n_lat.bit_length() - 1
    bit = [(lat // 2**s) % 2 for s in range(stages)]

    barrier = pltpu.get_barrier_semaphore()
    for k in range(1, n_lat):
        pl.semaphore_signal(
            barrier, inc=1, device_id={"lat": lax.rem(lat + k, n_lat)}, device_id_type=MESH
        )
    for k in range(1, n_lon):
        pl.semaphore_signal(
            barrier, inc=1, device_id={"lon": lax.rem(lon + k, n_lon)}, device_id_type=MESH
        )
    pl.semaphore_wait(barrier, n_lat + n_lon - 2)

    base = [0]
    for s in range(stages):
        base.append(base[-1] + n_lat // 2 ** (s + 1))

    def rows_of(r):
        block = lat
        for s in range(stages):
            if (r >> s) & 1:
                block = block + 2**s * (1 - 2 * bit[s])
        return pl.ds(pl.multiple_of(block * rows, 16), rows)

    def copy(s, slot):
        k = base[s] + slot
        return pltpu.make_async_remote_copy(
            src_ref=send.at[k],
            dst_ref=recv.at[k],
            send_sem=send_sem.at[k],
            recv_sem=recv_sem.at[k],
            device_id={"lat": lat + 2**s * (1 - 2 * bit[s])},
            device_id_type=MESH,
        )

    for slot in slots_in_order(stages - 1):
        send[base[0] + slot] = grad[rows_of(2 * slot + 1), :].astype(jnp.bfloat16)
        copy(0, slot).start()
    for s in range(stages):
        for slot in slots_in_order(stages - 1 - s):
            copy(s, slot).wait_recv()
            got = recv[base[s] + slot].astype(jnp.float32)
            r = slot << (s + 1)
            value = got + (grad[rows_of(r), :] if s == 0 else acc[r >> 1])
            if s + 1 == stages:
                beside[lon] = value.astype(jnp.bfloat16)
            elif slot % 2:
                send[base[s + 1] + slot // 2] = value.astype(jnp.bfloat16)
                copy(s + 1, slot // 2).start()
            else:
                acc[r >> 1] = value

    def lon_copy(k, source):
        return pltpu.make_async_remote_copy(
            src_ref=beside.at[source],
            dst_ref=beside.at[source],
            send_sem=lon_send.at[k],
            recv_sem=lon_recv.at[source],
            device_id={"lon": lax.rem(lon + k, n_lon)},
            device_id_type=MESH,
        )

    for k in range(1, n_lon):
        lon_copy(k, lon).start()
    for k in range(1, n_lon):
        lon_copy(k, lax.rem(lon + k, n_lon)).wait_recv()
    summed = beside[0].astype(jnp.float32)
    for k in range(1, n_lon):
        summed = summed + beside[k].astype(jnp.float32)
    direction[...] = summed

    square = jnp.sum((summed * summed).reshape(rows // 8, 8, channels), axis=0)
    part = square[:, :128]
    for c in range(128, channels, 128):
        part = part + square[:, c : c + 128]
    squares[lat] = part

    def square_copy(k, source):
        return pltpu.make_async_remote_copy(
            src_ref=squares.at[source],
            dst_ref=squares.at[source],
            send_sem=sq_send.at[k],
            recv_sem=sq_recv.at[source],
            device_id={"lat": lax.rem(lat + k, n_lat)},
            device_id_type=MESH,
        )

    for k in range(1, n_lat):
        square_copy(k, lat).start()
    for k in range(1, n_lat):
        square_copy(k, lax.rem(lat + k, n_lat)).wait_recv()
    total = jnp.sum(jnp.sum(squares[...], axis=0), keepdims=True)
    scaled = direction[...] / jnp.sqrt(total / count + 1e-06)
    direction[...] = scaled
    perturbed[...] = own[...].astype(jnp.float32) + 0.05 / count**0.5 * scaled

    for s in range(stages):
        for slot in range(n_lat >> (s + 1)):
            copy(s, slot).wait_send()
    for k in range(1, n_lon):
        lon_copy(k, lon).wait_send()
    for k in range(1, n_lat):
        square_copy(k, lat).wait_send()


def reduce_and_scale(grad, own, count):
    n_lat, n_lon = lax.axis_size("lat"), lax.axis_size("lon")
    rows, channels = own.shape
    block = jax.ShapeDtypeStruct((rows, channels), jnp.float32)
    vmem = pl.BlockSpec(memory_space=pltpu.VMEM)
    return pl.pallas_call(
        functools.partial(reduce_kernel, n_lat, n_lon, count),
        out_shape=(block, block),
        in_specs=[vmem, vmem],
        out_specs=(vmem, vmem),
        scratch_shapes=[
            pltpu.VMEM((n_lat // 2, rows, channels), jnp.float32),
            pltpu.VMEM((n_lat - 1, rows, channels), jnp.bfloat16),
            pltpu.VMEM((n_lat - 1, rows, channels), jnp.bfloat16),
            pltpu.VMEM((n_lon, rows, channels), jnp.bfloat16),
            pltpu.VMEM((n_lat, 8, 128), jnp.float32),
            pltpu.SemaphoreType.DMA((n_lat - 1,)),
            pltpu.SemaphoreType.DMA((n_lat - 1,)),
            pltpu.SemaphoreType.DMA((n_lon,)),
            pltpu.SemaphoreType.DMA((n_lon,)),
            pltpu.SemaphoreType.DMA((n_lat,)),
            pltpu.SemaphoreType.DMA((n_lat,)),
        ],
        compiler_params=pltpu.CompilerParams(
            collective_id=0, has_side_effects=True, vmem_limit_bytes=48 * 2**20
        ),
    )(grad, own)


def shards(features, upstream, kernel):
    height, breadth, channels = features.shape
    wide = 3 * channels
    wide_cols = padded_2(features, (("lon", 1),), 1, True)
    padded_x = padded_2(wide_cols, (("lat", 0),), 1, False)
    beside = jnp.concatenate([padded_x[:, b : b + breadth] for b in range(3)], axis=2)
    beside = beside.reshape((height + 2) * breadth, wide)
    views = [beside[a * breadth : (a + height) * breadth] for a in range(3)]
    z = sum(
        jnp.dot(views[a], kernel[a * wide : (a + 1) * wide], preferred_element_type=jnp.float32)
        for a in range(3)
    )
    slope = gated(upstream.reshape(-1, channels), z).astype(jnp.bfloat16)
    local_grad = jnp.concatenate(
        [
            lax.dot_general(
                view, slope, (((0,), (0,)), ((), ())), preferred_element_type=jnp.float32
            )
            for view in views
        ],
        axis=0,
    )
    slope = slope.reshape(height, breadth, channels)
    slope_cols = padded_2(slope, (("lon", 1),), 1, True)
    padded_slope = padded_2(slope_cols, (("lat", 0),), 1, False)
    back = lax.conv_general_dilated(
        padded_slope[None],
        kernel.reshape(3, 3, channels, channels)[::-1, ::-1],
        (1, 1),
        "VALID",
        dimension_numbers=("NHWC", "HWOI", "NHWC"),
        preferred_element_type=jnp.float32,
    )[0]
    input_grad = (upstream.astype(jnp.float32) + back).astype(jnp.bfloat16)
    count = 9.0 * channels * channels
    block_rows = kernel.shape[0] // lax.axis_size("lat")
    start = lax.axis_index("lat") * block_rows
    own_kernel = lax.dynamic_slice_in_dim(kernel, start, block_rows, 0)
    direction, perturbed = reduce_and_scale(local_grad, own_kernel, count)
    return (input_grad, direction, perturbed)


def solution(mesh):
    return jax.shard_map(
        shards,
        mesh=mesh,
        in_specs=(P("lat", "lon", None), P("lat", "lon", None), P()),
        out_specs=(P("lat", "lon", None), P("lat", None), P("lat", None)),
        check_vma=False,
    )
```

```python
import functools

import jax
import jax.numpy as jnp
from jax import lax
from jax.experimental import pallas as pl
from jax.experimental.pallas import tpu as pltpu
from jax.sharding import PartitionSpec as P

MESH = pl.DeviceIdType.MESH


def padded_2(block, sides, width, periodic):
    for axis, dim in sides:
        count = lax.axis_size(axis)
        forward = [(i, i + 1) for i in range(count - 1)]
        if periodic:
            forward.append((count - 1, 0))
        backward = [(target, source) for source, target in forward]
        low = lax.ppermute(
            lax.slice_in_dim(block, block.shape[dim] - width, None, axis=dim), axis, forward
        )
        high = lax.ppermute(lax.slice_in_dim(block, 0, width, axis=dim), axis, backward)
        block = jnp.concatenate([low, block, high], axis=dim)
    return block


def gated(upstream, z):
    sig = jax.nn.sigmoid(z)
    return upstream.astype(jnp.float32) * sig * (1.0 + z * (1.0 - sig))


def slots_in_order(bits):
    order = [0]
    for _ in range(bits):
        order = [2 * v for v in order] + [2 * v + 1 for v in order]
    reverse = lambda v: int(format(v, "b").zfill(bits)[::-1], 2) if bits else 0
    return sorted(order, key=reverse, reverse=True)


def reduce_kernel(n_lat, n_lon, count, *refs):
    parts, own, direction, perturbed = refs[:3], refs[3], refs[4], refs[5]
    grad, acc, send, recv, beside, squares = refs[6:12]
    send_sem, recv_sem, lon_send, lon_recv, sq_send, sq_recv, load_sem = refs[12:]
    rows, channels = own.shape
    pieces = send_sem.shape[1]
    width = channels // pieces
    part_rows = parts[0].shape[0]
    loads = [
        pltpu.make_async_copy(
            part, grad.at[pl.ds(a * part_rows, part_rows)], load_sem.at[a]
        )
        for a, part in enumerate(parts)
    ]
    for load in loads:
        load.start()
    lat = lax.axis_index("lat")
    lon = lax.axis_index("lon")
    stages = n_lat.bit_length() - 1
    bit = [(lat // 2**s) % 2 for s in range(stages)]

    barrier = pltpu.get_barrier_semaphore()
    for k in range(1, n_lat):
        pl.semaphore_signal(
            barrier, inc=1, device_id={"lat": lax.rem(lat + k, n_lat)}, device_id_type=MESH
        )
    for k in range(1, n_lon):
        pl.semaphore_signal(
            barrier, inc=1, device_id={"lon": lax.rem(lon + k, n_lon)}, device_id_type=MESH
        )
    pl.semaphore_wait(barrier, n_lat + n_lon - 2)
    for load in loads:
        load.wait()

    base = [0]
    for s in range(stages):
        base.append(base[-1] + n_lat // 2 ** (s + 1))

    def rows_of(r):
        block = lat
        for s in range(stages):
            if (r >> s) & 1:
                block = block + 2**s * (1 - 2 * bit[s])
        return pl.ds(pl.multiple_of(block * rows, 16), rows)

    def columns(piece):
        return pl.ds(piece * width, width)

    def copy(s, slot, piece):
        k = base[s] + slot
        return pltpu.make_async_remote_copy(
            src_ref=send.at[k, :, columns(piece)],
            dst_ref=recv.at[k, :, columns(piece)],
            send_sem=send_sem.at[k, piece],
            recv_sem=recv_sem.at[k, piece],
            device_id={"lat": lat + 2**s * (1 - 2 * bit[s])},
            device_id_type=MESH,
        )

    def lon_copy(k, source, piece):
        return pltpu.make_async_remote_copy(
            src_ref=beside.at[source, :, columns(piece)],
            dst_ref=beside.at[source, :, columns(piece)],
            send_sem=lon_send.at[k, piece],
            recv_sem=lon_recv.at[source, piece],
            device_id={"lon": lax.rem(lon + k, n_lon)},
            device_id_type=MESH,
        )

    def pass_on(s, slot, piece, value):
        send[base[s] + slot, :, columns(piece)] = value.astype(jnp.bfloat16)
        copy(s, slot, piece).start()

    for slot in slots_in_order(stages - 1):
        for piece in range(pieces):
            pass_on(0, slot, piece, grad[rows_of(2 * slot + 1), columns(piece)])
    for s in range(stages):
        for slot in slots_in_order(stages - 1 - s):
            for piece in range(pieces):
                copy(s, slot, piece).wait_recv()
                cols = columns(piece)
                got = recv[base[s] + slot, :, cols].astype(jnp.float32)
                r = slot << (s + 1)
                value = got + (grad[rows_of(r), cols] if s == 0 else acc[r >> 1, :, cols])
                if s + 1 == stages:
                    beside[lon, :, cols] = value.astype(jnp.bfloat16)
                    for k in range(1, n_lon):
                        lon_copy(k, lon, piece).start()
                elif slot % 2:
                    pass_on(s + 1, slot // 2, piece, value)
                else:
                    acc[r >> 1, :, cols] = value
    for piece in range(pieces):
        for k in range(1, n_lon):
            lon_copy(k, lax.rem(lon + k, n_lon), piece).wait_recv()
    summed = beside[0].astype(jnp.float32)
    for k in range(1, n_lon):
        summed = summed + beside[k].astype(jnp.float32)
    direction[...] = summed

    square = jnp.sum((summed * summed).reshape(rows // 8, 8, channels), axis=0)
    part = square[:, :128]
    for c in range(128, channels, 128):
        part = part + square[:, c : c + 128]
    squares[lat] = part

    def square_copy(k, source):
        return pltpu.make_async_remote_copy(
            src_ref=squares.at[source],
            dst_ref=squares.at[source],
            send_sem=sq_send.at[k],
            recv_sem=sq_recv.at[source],
            device_id={"lat": lax.rem(lat + k, n_lat)},
            device_id_type=MESH,
        )

    for k in range(1, n_lat):
        square_copy(k, lat).start()
    for k in range(1, n_lat):
        square_copy(k, lax.rem(lat + k, n_lat)).wait_recv()
    total = jnp.sum(jnp.sum(squares[...], axis=0), keepdims=True)
    scaled = direction[...] / jnp.sqrt(total / count + 1e-06)
    direction[...] = scaled
    perturbed[...] = own[...].astype(jnp.float32) + 0.05 / count**0.5 * scaled

    for piece in range(pieces):
        for s in range(stages):
            for slot in range(n_lat >> (s + 1)):
                copy(s, slot, piece).wait_send()
        for k in range(1, n_lon):
            lon_copy(k, lon, piece).wait_send()
    for k in range(1, n_lat):
        square_copy(k, lat).wait_send()


def reduce_and_scale(grads, own, count, pieces=2):
    n_lat, n_lon = lax.axis_size("lat"), lax.axis_size("lon")
    rows, channels = own.shape
    block = jax.ShapeDtypeStruct((rows, channels), jnp.float32)
    vmem = pl.BlockSpec(memory_space=pltpu.VMEM)
    return pl.pallas_call(
        functools.partial(reduce_kernel, n_lat, n_lon, count),
        out_shape=(block, block),
        in_specs=[pl.BlockSpec(memory_space=pl.ANY)] * 3 + [vmem],
        out_specs=(vmem, vmem),
        scratch_shapes=[
            pltpu.VMEM((rows * n_lat, channels), jnp.float32),
            pltpu.VMEM((n_lat // 2, rows, channels), jnp.float32),
            pltpu.VMEM((n_lat - 1, rows, channels), jnp.bfloat16),
            pltpu.VMEM((n_lat - 1, rows, channels), jnp.bfloat16),
            pltpu.VMEM((n_lon, rows, channels), jnp.bfloat16),
            pltpu.VMEM((n_lat, 8, 128), jnp.float32),
            pltpu.SemaphoreType.DMA((n_lat - 1, pieces)),
            pltpu.SemaphoreType.DMA((n_lat - 1, pieces)),
            pltpu.SemaphoreType.DMA((n_lon, pieces)),
            pltpu.SemaphoreType.DMA((n_lon, pieces)),
            pltpu.SemaphoreType.DMA((n_lat,)),
            pltpu.SemaphoreType.DMA((n_lat,)),
            pltpu.SemaphoreType.DMA((3,)),
        ],
        compiler_params=pltpu.CompilerParams(
            collective_id=0, has_side_effects=True, vmem_limit_bytes=48 * 2**20
        ),
    )(*grads, own)


def shards(features, upstream, kernel):
    height, breadth, channels = features.shape
    wide = 3 * channels
    wide_cols = padded_2(features, (("lon", 1),), 1, True)
    padded_x = padded_2(wide_cols, (("lat", 0),), 1, False)
    beside = jnp.concatenate([padded_x[:, b : b + breadth] for b in range(3)], axis=2)
    beside = beside.reshape((height + 2) * breadth, wide)
    views = [beside[a * breadth : (a + height) * breadth] for a in range(3)]
    z = sum(
        jnp.dot(views[a], kernel[a * wide : (a + 1) * wide], preferred_element_type=jnp.float32)
        for a in range(3)
    )
    slope = gated(upstream.reshape(-1, channels), z).astype(jnp.bfloat16)
    local_grads = [
        lax.dot_general(view, slope, (((0,), (0,)), ((), ())), preferred_element_type=jnp.float32)
        for view in views
    ]
    slope = slope.reshape(height, breadth, channels)
    slope_cols = padded_2(slope, (("lon", 1),), 1, True)
    padded_slope = padded_2(slope_cols, (("lat", 0),), 1, False)
    back = lax.conv_general_dilated(
        padded_slope[None],
        kernel.reshape(3, 3, channels, channels)[::-1, ::-1],
        (1, 1),
        "VALID",
        dimension_numbers=("NHWC", "HWOI", "NHWC"),
        preferred_element_type=jnp.float32,
    )[0]
    input_grad = (upstream.astype(jnp.float32) + back).astype(jnp.bfloat16)
    count = 9.0 * channels * channels
    block_rows = kernel.shape[0] // lax.axis_size("lat")
    start = lax.axis_index("lat") * block_rows
    own_kernel = lax.dynamic_slice_in_dim(kernel, start, block_rows, 0)
    direction, perturbed = reduce_and_scale(local_grads, own_kernel, count)
    return (input_grad, direction, perturbed)


def solution(mesh):
    return jax.shard_map(
        shards,
        mesh=mesh,
        in_specs=(P("lat", "lon", None), P("lat", "lon", None), P()),
        out_specs=(P("lat", "lon", None), P("lat", None), P("lat", None)),
        check_vma=False,
    )
```
